32 devices in a mesh: section: 4 (over y, x), seq: 2 (over core), exp: 4 (over z).
Axes of the slice: x: 2, y: 2, z: 4, core: 2. Of those that a mesh axis runs over, the one named last changes fastest.
Arguments:
- latent: bfloat16 [8, 8, 64, 384], P('section', 'seq', 'exp'), may hold values from -6 to 6
- cotangent: bfloat16 [8, 8, 64, 384], P('section', 'seq', 'exp'), may hold values from -6 to 6
- gain_one: float32 [384], replicated, may hold values from 0.5 to 2
- gain_two: float32 [384], replicated, may hold values from 0.5 to 2
- kernel_one: bfloat16 [3, 3, 3, 384, 384], P(None, None, None, 'exp'), may hold values from -0.0625 to 0.0625
- kernel_two: bfloat16 [3, 3, 3, 384, 384], P(None, None, None, 'exp'), may hold values from -0.0625 to 0.0625
Outputs:
- block_out: bfloat16 [8, 8, 64, 384], P('section', 'seq', 'exp')
- latent_grad: bfloat16 [8, 8, 64, 384], P('section', 'seq', 'exp')
The draws below stay inside these ranges and needn't reach their ends.
All inputs are finite; a program needn't handle non-finite values.
Results may differ from the reference program's by a relative error of at most 0.015.
Values may be sent and summed in bfloat16 or wider, within the bound.
A program may use at most 64 MiB of HBM per device.

```python
import math
import jax
import jax.numpy as jnp
from jax import lax

C = 384
NT = 8
NH = 8
NW = 64


def block_levels(rng, shape, pieces, least, top_value):
    loudness, own = 1.0, jax.random.fold_in(rng, 6)
    for position, parts in pieces:
        draws = jnp.exp(jax.random.uniform(jax.random.fold_in(own, position), (parts,), jnp.float32, least / len(pieces), top_value / len(pieces)))
        loudness = loudness * jnp.repeat(draws, shape[position] // parts).reshape([-1 if axis == position else 1 for axis in range(len(shape))])
    return loudness


def bell_draw(rng, shape, spread, limit, pieces=(), kind=jnp.bfloat16):
    loudness = block_levels(rng, shape, pieces, -0.22, 0.18) if pieces else 1.0
    array = jax.random.normal(rng, shape, jnp.float32) * spread * loudness
    return jnp.minimum(jnp.maximum(array, -limit), limit).astype(kind)


def setup_inputs(seed: int = 0) -> dict:
    keys = jax.random.split(jax.random.key(seed), 7)
    return {
        "latent": bell_draw(keys[0], (NT, NH, NW, C), 1.0, 6.0, ((0, 4), (1, 2), (2, 4))),
        "cotangent": bell_draw(keys[1], (NT, NH, NW, C), 1.0, 6.0, ((0, 4), (1, 2), (2, 4))),
        "gain_one": jnp.clip(jnp.exp(jax.random.uniform(keys[2], (C,), jnp.float32, math.log(0.5), math.log(2.0))), 0.5, 2.0),
        "gain_two": jnp.clip(jnp.exp(jax.random.uniform(keys[3], (C,), jnp.float32, math.log(0.5), math.log(2.0))), 0.5, 2.0),
        "kernel_one": bell_draw(keys[4], (3, 3, 3, C, C), (27 * C) ** -0.5, 0.0625, ((3, 4),)),
        "kernel_two": bell_draw(keys[5], (3, 3, 3, C, C), (27 * C) ** -0.5, 0.0625, ((3, 4),)),
    }


epsilon = 1e-06

def normalize(values, gain):
    inverse = lax.rsqrt(lax.optimization_barrier(jnp.mean(values * values, axis=-1, keepdims=True)) + epsilon)
    return (values * inverse * gain, inverse)

def norm_backward(values, inverse, gain, upstream):
    scaled = upstream * gain
    return inverse * scaled - values * inverse ** 3 * lax.optimization_barrier(jnp.mean(values * scaled, axis=-1, keepdims=True))

def silu_slope(normed):
    sigma = jax.nn.sigmoid(normed)
    return sigma * (1.0 + normed * (1.0 - sigma))

def forward_kernel(weight):
    swapped = jnp.swapaxes(weight, 3, 4)
    return swapped.reshape(3, 3, 3 * swapped.shape[3], swapped.shape[4])

def backward_kernel(weight):
    flipped = weight[::-1, ::-1, ::-1]
    return flipped.reshape(3, 3, 3 * flipped.shape[3], flipped.shape[4])

def conv_taps(padded, kernel, frame_count, row_count, col_count):
    summed = jnp.zeros((frame_count * row_count * col_count, kernel.shape[3]), jnp.float32)
    for time_tap in range(3):
        for row_tap in range(3):
            columns = jnp.concatenate([padded[time_tap:time_tap + frame_count, row_tap:row_tap + row_count, col_tap:col_tap + col_count] for col_tap in range(3)], axis=-1)
            columns = columns.reshape(frame_count * row_count * col_count, columns.shape[-1])
            summed = summed + jnp.dot(columns, kernel[time_tap, row_tap], preferred_element_type=jnp.float32)
    return summed.reshape(frame_count, row_count, col_count, kernel.shape[3])

def conv_whole(padded, kernel):

    def one_frame(index):
        window = lax.dynamic_slice_in_dim(padded, index, 3, 0)
        return conv_taps(window, kernel, 1, NH, NW)[0]
    return lax.map(one_frame, jnp.arange(NT, dtype=jnp.int32))

def reference(latent, cotangent, gain_one, gain_two, kernel_one, kernel_two):
    ahead = ((2, 0), (1, 1), (1, 1), (0, 0))
    behind = ((0, 2), (1, 1), (1, 1), (0, 0))
    source = latent.astype(jnp.float32)
    normed_one, inverse_one = normalize(source, gain_one)
    active_one = jax.nn.silu(normed_one).astype(jnp.bfloat16)
    inner = conv_whole(jnp.pad(active_one, ahead), forward_kernel(kernel_one))
    normed_two, inverse_two = normalize(inner, gain_two)
    active_two = jax.nn.silu(normed_two).astype(jnp.bfloat16)
    branch = conv_whole(jnp.pad(active_two, ahead), forward_kernel(kernel_two))
    block_out = (source + branch).astype(jnp.bfloat16)
    grad_two = conv_whole(jnp.pad(cotangent, behind), backward_kernel(kernel_two))
    grad_inner = norm_backward(inner, inverse_two, gain_two, grad_two * silu_slope(normed_two)).astype(jnp.bfloat16)
    grad_one = conv_whole(jnp.pad(grad_inner, behind), backward_kernel(kernel_one))
    latent_grad = cotangent.astype(jnp.float32) + norm_backward(source, inverse_one, gain_one, grad_one * silu_slope(normed_one))
    return (block_out, latent_grad.astype(jnp.bfloat16))
```

```python
import functools

import jax
import jax.numpy as jnp
from jax import lax
from jax.experimental import pallas as pl
from jax.experimental.pallas import tpu as pltpu
from jax.sharding import PartitionSpec as P

epsilon = 1e-06
MESH = pl.DeviceIdType.MESH
bf16, f32 = jnp.bfloat16, jnp.float32


def normalize(values, gain):
    inverse = lax.rsqrt(jnp.mean(values * values, axis=-1, keepdims=True) + epsilon)
    return values * inverse * gain, inverse


def norm_backward(values, inverse, gain, upstream):
    scaled = upstream * gain
    mean = jnp.mean(values * scaled, axis=-1, keepdims=True)
    return inverse * scaled - values * (inverse * inverse * inverse) * mean


def silu(normed):
    return normed / (1.0 + jnp.exp(-normed))


def silu_slope(normed):
    sigma = 1.0 / (1.0 + jnp.exp(-normed))
    return sigma * (1.0 + normed * (1.0 - sigma))


def shift_sum(taps, width, size):
    rows = taps.shape[0]
    column = lax.rem(lax.broadcasted_iota(jnp.int32, (rows, size), 0), width)
    low = pltpu.roll(taps[:, :size], 1, axis=0)
    high = pltpu.roll(taps[:, 2 * size :], rows - 1, axis=0)
    return (
        taps[:, size : 2 * size]
        + jnp.where(column == 0, 0.0, low)
        + jnp.where(column == width - 1, 0.0, high)
    )


def stage(index, sizes, act, grad, w_fwd, w_bwd, bufs, send, recv, w_ready):
    S, Q, Z = sizes
    xp, qs, qp, yf, rf, rp, yb, rb = bufs
    F, R, W, C = act.shape
    O = w_fwd.shape[3]
    WW = W * Z
    OP = -(-O // 128) * 128
    s, q, z = lax.axis_index("section"), lax.axis_index("seq"), lax.axis_index("exp")
    has_next, has_prev = s < S - 1, s > 0
    has_high, has_low = q < Q - 1, q > 0
    nxt, prv = jnp.minimum(s + 1, S - 1), jnp.maximum(s - 1, 0)
    upper, lower = jnp.minimum(q + 1, Q - 1), jnp.maximum(q - 1, 0)
    mine = pl.ds(pl.multiple_of(z * W, W), W)
    body = pl.ds(1, R)

    def peer(d):
        return lax.rem(z + d, Z)

    def columns(d):
        return pl.ds(pl.multiple_of(peer(d) * W, W), W)

    def remote(src, dst, slot, device):
        return pltpu.make_async_remote_copy(
            src_ref=src,
            dst_ref=dst,
            send_sem=send.at[index, slot],
            recv_sem=recv.at[index, slot],
            device_id=device,
            device_id_type=MESH,
        )

    def q_own(d):
        return remote(qs.at[peer(d)], qp.at[pl.ds(0, F), body, mine], d, (s, q, peer(d)))

    def q_prev(d):
        return remote(
            qs.at[peer(d), pl.ds(0, 2)], qp.at[pl.ds(F, 2), body, mine], Z + d, (prv, q, peer(d))
        )

    def x_own(d):
        return remote(act, xp.at[:, body, mine], 2 * Z + d, (s, q, peer(d)))

    def b_own(d):
        return remote(yb.at[:, :, columns(d)], rb.at[d], 3 * Z + d, (s, q, peer(d)))

    def f_own(d):
        return remote(
            yf.at[pl.ds(0, F), :, columns(d)], rf.at[z], 4 * Z + d, (s, q, peer(d))
        )

    def f_next(d):
        return remote(
            yf.at[pl.ds(F, 2), :, columns(d)], rp.at[z], 5 * Z + d, (nxt, q, peer(d))
        )

    def to_high(buf, slot):
        return remote(buf.at[:, R], buf.at[:, 0], slot, (s, upper, z))

    def to_low(buf, slot):
        return remote(buf.at[:, 1], buf.at[:, R + 1], slot, (s, lower, z))

    def exchange_rows(buf, slot):
        @pl.when(has_high)
        def _():
            to_high(buf, slot).start()

        @pl.when(has_low)
        def _():
            to_low(buf, slot + 1).start()

        @pl.when(jnp.logical_not(has_low))
        def _():
            buf[:, 0] = jnp.zeros_like(buf[:, 0])

        @pl.when(jnp.logical_not(has_high))
        def _():
            buf[:, R + 1] = jnp.zeros_like(buf[:, R + 1])

        @pl.when(has_low)
        def _():
            to_high(buf, slot).wait_recv()

        @pl.when(has_high)
        def _():
            to_low(buf, slot + 1).wait_recv()

    for m in range(Z):
        qs[m] = grad[:, :, :, m * O : (m + 1) * O]
    for d in range(1, Z):
        q_own(d).start()

    @pl.when(has_prev)
    def _():
        for d in range(Z):
            q_prev(d).start()

    for d in range(1, Z):
        x_own(d).start()
    qp[pl.ds(0, F), body, mine] = qs[z]
    xp[:, body, mine] = act[...]

    @pl.when(jnp.logical_not(has_next))
    def _():
        qp[pl.ds(F, 2), body] = jnp.zeros((2, R, WW, O), bf16)

    for d in range(1, Z):
        q_own(d).wait_recv()

    @pl.when(has_next)
    def _():
        for d in range(Z):
            q_prev(d).wait_recv()

    exchange_rows(qp, 6 * Z)
    w_ready[1].wait()

    def padded(value, axis):
        shape = list(value.shape)
        shape[axis] = OP - O
        if OP == O:
            return value
        return jnp.concatenate([value, jnp.zeros(shape, value.dtype)], axis=axis)

    for f in range(F):
        total = None
        for i in range(3):
            lhs = jnp.concatenate(
                [padded(qp[f + i, pl.ds(j, R)].reshape(R * WW, O), 1) for j in range(3)], axis=1
            )
            rhs = jnp.concatenate(
                [
                    jnp.concatenate(
                        [padded(w_bwd[2 - i, 2 - j, 2 - l], 0) for l in range(3)], axis=1
                    )
                    for j in range(3)
                ],
                axis=0,
            )
            part = jnp.dot(lhs, rhs, preferred_element_type=f32)
            total = part if total is None else total + part
        yb[f] = shift_sum(total, WW, C).astype(bf16).reshape(R, WW, C)
    for d in range(1, Z):
        b_own(d).start()

    for d in range(1, Z):
        x_own(d).wait_recv()
    exchange_rows(xp, 6 * Z + 2)
    w_ready[0].wait()
    for t in list(range(F, F + 2)) + list(range(F)):
        total = None
        for i in range(3):
            f = t + i - 2
            if not 0 <= f < F:
                continue
            lhs = jnp.concatenate(
                [xp[f, pl.ds(j, R)].reshape(R * WW, C) for j in range(3)], axis=1
            )
            rhs = jnp.concatenate(
                [
                    jnp.concatenate([padded(w_fwd[i, j, l], 0) for l in range(3)], axis=0)
                    for j in range(3)
                ],
                axis=1,
            )
            part = lax.dot_general(
                lhs, rhs, (((1,), (1,)), ((), ())), preferred_element_type=f32
            )
            total = part if total is None else total + part
        yf[t] = shift_sum(total, WW, OP)[:, :O].astype(bf16).reshape(R, WW, O)
        if t == F + 1:

            @pl.when(has_next)
            def _():
                for d in range(Z):
                    f_next(d).start()

    for d in range(1, Z):
        f_own(d).start()
    rf[z] = yf[pl.ds(0, F), :, mine]

    @pl.when(jnp.logical_not(has_prev))
    def _():
        rp[...] = jnp.zeros_like(rp)

    for d in range(1, Z):
        b_own(d).wait_recv()
    result_b = yb[:, :, mine].astype(f32)
    for d in range(1, Z):
        result_b = result_b + rb[d].astype(f32)
    result_b = result_b.reshape(F * R * W, C)

    for d in range(1, Z):
        f_own(d).wait_recv()

    @pl.when(has_prev)
    def _():
        for d in range(Z):
            f_next(d).wait_recv()

    chunks = []
    for m in range(Z):
        head = rf[m, pl.ds(0, 2)].astype(f32) + rp[m].astype(f32)
        if F > 2:
            head = jnp.concatenate([head, rf[m, pl.ds(2, F - 2)].astype(f32)], axis=0)
        chunks.append(head.reshape(F * R * W, O))
    result_f = jnp.concatenate(chunks, axis=1)

    def drain():
        for d in range(1, Z):
            q_own(d).wait_send()
            x_own(d).wait_send()
            b_own(d).wait_send()
            f_own(d).wait_send()

        @pl.when(has_prev)
        def _():
            for d in range(Z):
                q_prev(d).wait_send()

        @pl.when(has_next)
        def _():
            for d in range(Z):
                f_next(d).wait_send()

        for buf, slot in ((qp, 6 * Z), (xp, 6 * Z + 2)):

            @pl.when(has_high)
            def _():
                to_high(buf, slot).wait_send()

            @pl.when(has_low)
            def _():
                to_low(buf, slot + 1).wait_send()

    return result_f, result_b, drain


def kernel(sizes, latent, cotangent, gain_one, gain_two, kernel_one, kernel_two, out, latent_grad, *scratch):
    S, Q, Z = sizes
    act_one, act_two, grad_two_ref, w_one, w_two, send, recv, w_sem = scratch[:8]
    bufs_one, bufs_two = scratch[8:16], scratch[16:24]
    F, R, W, C = latent.shape
    rows = F * R * W
    s, q, z = lax.axis_index("section"), lax.axis_index("seq"), lax.axis_index("exp")

    load_one = pltpu.make_async_copy(kernel_one, w_one, w_sem.at[0])
    load_two = pltpu.make_async_copy(kernel_two, w_two, w_sem.at[1])
    load_two.start()
    load_one.start()

    barrier = pltpu.get_barrier_semaphore()

    def greet(device):
        pl.semaphore_signal(barrier, inc=1, device_id=device, device_id_type=MESH)

    for d in range(1, Z):
        greet((s, q, lax.rem(z + d, Z)))
    for condition, step in ((s < S - 1, 1), (s > 0, -1)):

        @pl.when(condition)
        def _():
            for d in range(Z):
                greet((s + step, q, lax.rem(z + d, Z)))

    for condition, step in ((q < Q - 1, 1), (q > 0, -1)):

        @pl.when(condition)
        def _():
            greet((s, q + step, z))

    source = latent[...].reshape(rows, C).astype(f32)
    g_one, g_two = gain_one[...], gain_two[...]
    normed_one, inverse_one = normalize(source, g_one)
    act_one[...] = silu(normed_one).astype(bf16).reshape(F, R, W, C)

    sections = (s < S - 1).astype(jnp.int32) + (s > 0).astype(jnp.int32)
    neighbours = (q < Q - 1).astype(jnp.int32) + (q > 0).astype(jnp.int32)
    pl.semaphore_wait(barrier, Z - 1 + Z * sections + neighbours)

    class Done:
        def wait(self):
            pass

    inner, grad_two, drain_one = stage(
        0, sizes, act_one, cotangent, w_one, w_two, bufs_one, send, recv, (load_one, load_two)
    )
    normed_two, inverse_two = normalize(inner, g_two)
    act_two[...] = silu(normed_two).astype(bf16).reshape(F, R, W, C)
    grad_inner = norm_backward(inner, inverse_two, g_two, grad_two * silu_slope(normed_two))
    grad_two_ref[...] = grad_inner.astype(bf16).reshape(F, R, W, C)

    branch, grad_one, drain_two = stage(
        1, sizes, act_two, grad_two_ref, w_two, w_one, bufs_two, send, recv, (Done(), Done())
    )
    source = latent[...].reshape(rows, C).astype(f32)
    out[...] = (source + branch).astype(bf16).reshape(F, R, W, C)
    normed_one, inverse_one = normalize(source, g_one)
    grad = norm_backward(source, inverse_one, g_one, grad_one * silu_slope(normed_one))
    upstream = cotangent[...].reshape(rows, C).astype(f32)
    latent_grad[...] = (upstream + grad).astype(bf16).reshape(F, R, W, C)
    drain_one()
    drain_two()


def local(sizes, latent, cotangent, gain_one, gain_two, kernel_one, kernel_two):
    S, Q, Z = sizes
    F, R, W, C = latent.shape
    O = kernel_one.shape[3]
    WW = W * Z
    block = pltpu.VMEM((F, R, W, C), bf16)
    weight = pltpu.VMEM(kernel_one.shape, bf16)
    bufs = [
        pltpu.VMEM((F, R + 2, WW, C), bf16),
        pltpu.VMEM((Z, F, R, W, O), bf16),
        pltpu.VMEM((F + 2, R + 2, WW, O), bf16),
        pltpu.VMEM((F + 2, R, WW, O), bf16),
        pltpu.VMEM((Z, F, R, W, O), bf16),
        pltpu.VMEM((Z, 2, R, W, O), bf16),
        pltpu.VMEM((F, R, WW, C), bf16),
        pltpu.VMEM((Z, F, R, W, C), bf16),
    ]
    slots = 6 * Z + 4
    vmem = pl.BlockSpec(memory_space=pltpu.VMEM)
    hbm = pl.BlockSpec(memory_space=pl.ANY)
    return pl.pallas_call(
        functools.partial(kernel, sizes),
        out_shape=[jax.ShapeDtypeStruct((F, R, W, C), bf16)] * 2,
        in_specs=[vmem, vmem, vmem, vmem, hbm, hbm],
        out_specs=[vmem, vmem],
        scratch_shapes=[
            block,
            block,
            block,
            weight,
            weight,
            pltpu.SemaphoreType.DMA((2, slots)),
            pltpu.SemaphoreType.DMA((2, slots)),
            pltpu.SemaphoreType.DMA((2,)),
            *bufs,
            *bufs,
        ],
        compiler_params=pltpu.CompilerParams(
            collective_id=0, has_side_effects=True, vmem_limit_bytes=60 * 1024 * 1024
        ),
    )(latent, cotangent, gain_one.reshape(1, C), gain_two.reshape(1, C), kernel_one, kernel_two)


def solution(mesh):
    sizes = (mesh.shape["section"], mesh.shape["seq"], mesh.shape["exp"])
    spread = P("section", "seq", "exp", None)
    split = P(None, None, None, "exp", None)
    return jax.shard_map(
        functools.partial(local, sizes),
        mesh=mesh,
        in_specs=(spread, spread, P(), P(), split, split),
        out_specs=(spread, spread),
        check_vma=False,
    )
```

```python
import functools

import jax
import jax.numpy as jnp
from jax import lax
from jax.experimental import pallas as pl
from jax.experimental.pallas import tpu as pltpu
from jax.sharding import PartitionSpec as P

epsilon = 1e-06
MESH = pl.DeviceIdType.MESH
bf16, f32 = jnp.bfloat16, jnp.float32


def normalize(values, gain):
    inverse = lax.rsqrt(jnp.mean(values * values, axis=-1, keepdims=True) + epsilon)
    return values * inverse * gain, inverse


def norm_backward(values, inverse, gain, upstream):
    scaled = upstream * gain
    mean = jnp.mean(values * scaled, axis=-1, keepdims=True)
    return inverse * scaled - values * (inverse * inverse * inverse) * mean


def silu(normed):
    return normed / (1.0 + jnp.exp(-normed))


def silu_slope(normed):
    sigma = 1.0 / (1.0 + jnp.exp(-normed))
    return sigma * (1.0 + normed * (1.0 - sigma))


def shift_sum(taps, width, size):
    rows = taps.shape[0]
    column = lax.rem(lax.broadcasted_iota(jnp.int32, (rows, size), 0), width)
    low = pltpu.roll(taps[:, :size], 1, axis=0)
    high = pltpu.roll(taps[:, 2 * size :], rows - 1, axis=0)
    return (
        taps[:, size : 2 * size]
        + jnp.where(column == 0, 0.0, low)
        + jnp.where(column == width - 1, 0.0, high)
    )


def stage(index, sizes, act, grad, w_fwd, w_bwd, bufs, send, recv, w_ready):
    S, Q, Z = sizes
    xp, qs, qp, yf, rf, rp, yb, rb = bufs
    F, R, W, C = act.shape
    O = w_fwd.shape[3]
    WW = W * Z
    OP = -(-O // 128) * 128
    s, q, z = lax.axis_index("section"), lax.axis_index("seq"), lax.axis_index("exp")
    has_next, has_prev = s < S - 1, s > 0
    has_high, has_low = q < Q - 1, q > 0
    nxt, prv = jnp.minimum(s + 1, S - 1), jnp.maximum(s - 1, 0)
    upper, lower = jnp.minimum(q + 1, Q - 1), jnp.maximum(q - 1, 0)
    mine = pl.ds(pl.multiple_of(z * W, W), W)
    body = pl.ds(1, R)

    def peer(d):
        return lax.rem(z + d, Z)

    def columns(d):
        return pl.ds(pl.multiple_of(peer(d) * W, W), W)

    def remote(src, dst, slot, device):
        return pltpu.make_async_remote_copy(
            src_ref=src,
            dst_ref=dst,
            send_sem=send.at[index, slot],
            recv_sem=recv.at[index, slot],
            device_id=device,
            device_id_type=MESH,
        )

    def q_own(d):
        return remote(qs.at[peer(d)], qp.at[pl.ds(0, F), body, mine], d, (s, q, peer(d)))

    def q_prev(d):
        return remote(
            qs.at[peer(d), pl.ds(0, 2)], qp.at[pl.ds(F, 2), body, mine], Z + d, (prv, q, peer(d))
        )

    def block_at(owner):
        return xp.at[:, body, pl.ds(pl.multiple_of(jnp.clip(owner, 0, Z - 1) * W, W), W)]

    def x_right(k):
        held = block_at(z - (k - 1))
        return remote(act if k == 1 else held, held, 2 * Z + k, (s, q, jnp.minimum(z + 1, Z - 1)))

    def x_left(k):
        held = block_at(z + (k - 1))
        return remote(act if k == 1 else held, held, 6 * Z + 4 + k, (s, q, jnp.maximum(z - 1, 0)))

    def sends_right(k):
        return jnp.logical_and(z >= k - 1, z < Z - 1)

    def sends_left(k):
        return jnp.logical_and(z <= Z - k, z > 0)

    def pass_on(k):
        @pl.when(sends_right(k))
        def _():
            x_right(k).start()

        @pl.when(sends_left(k))
        def _():
            x_left(k).start()

    def arrive(k):
        @pl.when(z >= k)
        def _():
            x_right(k).wait_recv()

        @pl.when(z <= Z - 1 - k)
        def _():
            x_left(k).wait_recv()

        if k < Z - 1:
            pass_on(k + 1)

    def b_own(d):
        return remote(yb.at[:, :, columns(d)], rb.at[d], 3 * Z + d, (s, q, peer(d)))

    def f_own(d):
        return remote(
            yf.at[pl.ds(0, F), :, columns(d)], rf.at[z], 4 * Z + d, (s, q, peer(d))
        )

    def f_next(d):
        return remote(
            yf.at[pl.ds(F, 2), :, columns(d)], rp.at[z], 5 * Z + d, (nxt, q, peer(d))
        )

    def to_high(buf, slot):
        return remote(buf.at[:, R], buf.at[:, 0], slot, (s, upper, z))

    def to_low(buf, slot):
        return remote(buf.at[:, 1], buf.at[:, R + 1], slot, (s, lower, z))

    def exchange_rows(buf, slot):
        @pl.when(has_high)
        def _():
            to_high(buf, slot).start()

        @pl.when(has_low)
        def _():
            to_low(buf, slot + 1).start()

        @pl.when(jnp.logical_not(has_low))
        def _():
            buf[:, 0] = jnp.zeros_like(buf[:, 0])

        @pl.when(jnp.logical_not(has_high))
        def _():
            buf[:, R + 1] = jnp.zeros_like(buf[:, R + 1])

        @pl.when(has_low)
        def _():
            to_high(buf, slot).wait_recv()

        @pl.when(has_high)
        def _():
            to_low(buf, slot + 1).wait_recv()

    for m in range(Z):
        qs[m] = grad[:, :, :, m * O : (m + 1) * O]
    for d in range(1, Z):
        q_own(d).start()

    @pl.when(has_prev)
    def _():
        for d in range(Z):
            q_prev(d).start()

    if Z > 1:
        pass_on(1)
    qp[pl.ds(0, F), body, mine] = qs[z]
    xp[:, body, mine] = act[...]

    @pl.when(jnp.logical_not(has_next))
    def _():
        qp[pl.ds(F, 2), body] = jnp.zeros((2, R, WW, O), bf16)

    for d in range(1, Z):
        q_own(d).wait_recv()

    @pl.when(has_next)
    def _():
        for d in range(Z):
            q_prev(d).wait_recv()

    exchange_rows(qp, 6 * Z)
    arrived = 1
    w_ready[1].wait()

    def padded(value, axis):
        shape = list(value.shape)
        shape[axis] = OP - O
        if OP == O:
            return value
        return jnp.concatenate([value, jnp.zeros(shape, value.dtype)], axis=axis)

    for f in range(F):
        if arrived < Z:
            arrive(arrived)
            arrived += 1
        total = None
        for i in range(3):
            lhs = jnp.concatenate(
                [padded(qp[f + i, pl.ds(j, R)].reshape(R * WW, O), 1) for j in range(3)], axis=1
            )
            rhs = jnp.concatenate(
                [
                    jnp.concatenate(
                        [padded(w_bwd[2 - i, 2 - j, 2 - l], 0) for l in range(3)], axis=1
                    )
                    for j in range(3)
                ],
                axis=0,
            )
            part = jnp.dot(lhs, rhs, preferred_element_type=f32)
            total = part if total is None else total + part
        yb[f] = shift_sum(total, WW, C).astype(bf16).reshape(R, WW, C)
    for d in range(1, Z):
        b_own(d).start()

    for k in range(arrived, Z):
        arrive(k)
    exchange_rows(xp, 6 * Z + 2)
    w_ready[0].wait()
    for t in list(range(F, F + 2)) + list(range(F)):
        total = None
        for i in range(3):
            f = t + i - 2
            if not 0 <= f < F:
                continue
            lhs = jnp.concatenate(
                [xp[f, pl.ds(j, R)].reshape(R * WW, C) for j in range(3)], axis=1
            )
            rhs = jnp.concatenate(
                [
                    jnp.concatenate([padded(w_fwd[i, j, l], 0) for l in range(3)], axis=0)
                    for j in range(3)
                ],
                axis=1,
            )
            part = lax.dot_general(
                lhs, rhs, (((1,), (1,)), ((), ())), preferred_element_type=f32
            )
            total = part if total is None else total + part
        yf[t] = shift_sum(total, WW, OP)[:, :O].astype(bf16).reshape(R, WW, O)
        if t == F + 1:

            @pl.when(has_next)
            def _():
                for d in range(Z):
                    f_next(d).start()

    for d in range(1, Z):
        f_own(d).start()
    rf[z] = yf[pl.ds(0, F), :, mine]

    @pl.when(jnp.logical_not(has_prev))
    def _():
        rp[...] = jnp.zeros_like(rp)

    for d in range(1, Z):
        b_own(d).wait_recv()
    result_b = yb[:, :, mine].astype(f32)
    for d in range(1, Z):
        result_b = result_b + rb[d].astype(f32)
    result_b = result_b.reshape(F * R * W, C)

    for d in range(1, Z):
        f_own(d).wait_recv()

    @pl.when(has_prev)
    def _():
        for d in range(Z):
            f_next(d).wait_recv()

    chunks = []
    for m in range(Z):
        head = rf[m, pl.ds(0, 2)].astype(f32) + rp[m].astype(f32)
        if F > 2:
            head = jnp.concatenate([head, rf[m, pl.ds(2, F - 2)].astype(f32)], axis=0)
        chunks.append(head.reshape(F * R * W, O))
    result_f = jnp.concatenate(chunks, axis=1)

    def drain():
        for k in range(1, Z):

            @pl.when(sends_right(k))
            def _():
                x_right(k).wait_send()

            @pl.when(sends_left(k))
            def _():
                x_left(k).wait_send()

        for d in range(1, Z):
            q_own(d).wait_send()
            b_own(d).wait_send()
            f_own(d).wait_send()

        @pl.when(has_prev)
        def _():
            for d in range(Z):
                q_prev(d).wait_send()

        @pl.when(has_next)
        def _():
            for d in range(Z):
                f_next(d).wait_send()

        for buf, slot in ((qp, 6 * Z), (xp, 6 * Z + 2)):

            @pl.when(has_high)
            def _():
                to_high(buf, slot).wait_send()

            @pl.when(has_low)
            def _():
                to_low(buf, slot + 1).wait_send()

    return result_f, result_b, drain


def kernel(sizes, latent, cotangent, gain_one, gain_two, kernel_one, kernel_two, out, latent_grad, *scratch):
    S, Q, Z = sizes
    act_one, act_two, grad_two_ref, w_one, w_two, send, recv, w_sem = scratch[:8]
    bufs_one, bufs_two = scratch[8:16], scratch[16:24]
    F, R, W, C = latent.shape
    rows = F * R * W
    s, q, z = lax.axis_index("section"), lax.axis_index("seq"), lax.axis_index("exp")

    load_one = pltpu.make_async_copy(kernel_one, w_one, w_sem.at[0])
    load_two = pltpu.make_async_copy(kernel_two, w_two, w_sem.at[1])
    load_two.start()
    load_one.start()

    barrier = pltpu.get_barrier_semaphore()

    def greet(device):
        pl.semaphore_signal(barrier, inc=1, device_id=device, device_id_type=MESH)

    for d in range(1, Z):
        greet((s, q, lax.rem(z + d, Z)))
    for condition, step in ((s < S - 1, 1), (s > 0, -1)):

        @pl.when(condition)
        def _():
            for d in range(Z):
                greet((s + step, q, lax.rem(z + d, Z)))

    for condition, step in ((q < Q - 1, 1), (q > 0, -1)):

        @pl.when(condition)
        def _():
            greet((s, q + step, z))

    source = latent[...].reshape(rows, C).astype(f32)
    g_one, g_two = gain_one[...].reshape(1, C), gain_two[...].reshape(1, C)
    normed_one, inverse_one = normalize(source, g_one)
    act_one[...] = silu(normed_one).astype(bf16).reshape(F, R, W, C)

    sections = (s < S - 1).astype(jnp.int32) + (s > 0).astype(jnp.int32)
    neighbours = (q < Q - 1).astype(jnp.int32) + (q > 0).astype(jnp.int32)
    pl.semaphore_wait(barrier, Z - 1 + Z * sections + neighbours)

    class Done:
        def wait(self):
            pass

    inner, grad_two, drain_one = stage(
        0, sizes, act_one, cotangent, w_one, w_two, bufs_one, send, recv, (load_one, load_two)
    )
    normed_two, inverse_two = normalize(inner, g_two)
    act_two[...] = silu(normed_two).astype(bf16).reshape(F, R, W, C)
    grad_inner = norm_backward(inner, inverse_two, g_two, grad_two * silu_slope(normed_two))
    grad_two_ref[...] = grad_inner.astype(bf16).reshape(F, R, W, C)

    branch, grad_one, drain_two = stage(
        1, sizes, act_two, grad_two_ref, w_two, w_one, bufs_two, send, recv, (Done(), Done())
    )
    source = latent[...].reshape(rows, C).astype(f32)
    out[...] = (source + branch).astype(bf16).reshape(F, R, W, C)
    normed_one, inverse_one = normalize(source, g_one)
    grad = norm_backward(source, inverse_one, g_one, grad_one * silu_slope(normed_one))
    upstream = cotangent[...].reshape(rows, C).astype(f32)
    latent_grad[...] = (upstream + grad).astype(bf16).reshape(F, R, W, C)
    drain_one()
    drain_two()


def local(sizes, latent, cotangent, gain_one, gain_two, kernel_one, kernel_two):
    S, Q, Z = sizes
    F, R, W, C = latent.shape
    O = kernel_one.shape[3]
    WW = W * Z
    block = pltpu.VMEM((F, R, W, C), bf16)
    weight = pltpu.VMEM(kernel_one.shape, bf16)
    bufs = [
        pltpu.VMEM((F, R + 2, WW, C), bf16),
        pltpu.VMEM((Z, F, R, W, O), bf16),
        pltpu.VMEM((F + 2, R + 2, WW, O), bf16),
        pltpu.VMEM((F + 2, R, WW, O), bf16),
        pltpu.VMEM((Z, F, R, W, O), bf16),
        pltpu.VMEM((Z, 2, R, W, O), bf16),
        pltpu.VMEM((F, R, WW, C), bf16),
        pltpu.VMEM((Z, F, R, W, C), bf16),
    ]
    slots = 7 * Z + 4
    vmem = pl.BlockSpec(memory_space=pltpu.VMEM)
    hbm = pl.BlockSpec(memory_space=pl.ANY)
    return pl.pallas_call(
        functools.partial(kernel, sizes),
        out_shape=[jax.ShapeDtypeStruct((F, R, W, C), bf16)] * 2,
        in_specs=[vmem, vmem, vmem, vmem, hbm, hbm],
        out_specs=[vmem, vmem],
        scratch_shapes=[
            block,
            block,
            block,
            weight,
            weight,
            pltpu.SemaphoreType.DMA((2, slots)),
            pltpu.SemaphoreType.DMA((2, slots)),
            pltpu.SemaphoreType.DMA((2,)),
            *bufs,
            *bufs,
        ],
        compiler_params=pltpu.CompilerParams(
            collective_id=0, has_side_effects=True, vmem_limit_bytes=60 * 1024 * 1024
        ),
    )(latent, cotangent, gain_one, gain_two, kernel_one, kernel_two)


def solution(mesh):
    sizes = (mesh.shape["section"], mesh.shape["seq"], mesh.shape["exp"])
    spread = P("section", "seq", "exp", None)
    split = P(None, None, None, "exp", None)
    return jax.shard_map(
        functools.partial(local, sizes),
        mesh=mesh,
        in_specs=(spread, spread, P(), P(), split, split),
        out_specs=(spread, spread),
        check_vma=False,
    )
```
